32 devices in a mesh: run: 2 (over y), gx: 4 (over x, core), gy: 4 (over z).
Axes of the slice: x: 2, y: 2, z: 4, core: 2. Of those that a mesh axis runs over, the one named last changes fastest.
Arguments:
- magnet: float32 [3, 4, 256, 256], P(None, None, ('run', 'gx', 'gy')), parts along dimension 2, may hold values from -1 to 1, as said below
- window_shift: int32 [2], P('run'), parts along dimension 0, may hold values from 1 to 7
- region: int32 [256, 256], P(('run', 'gx', 'gy')), parts along dimension 0, may hold values 0 or 1
- material: float32 [4, 5], replicated, may hold values from 0.1 to 1
- kernel: float32 [6, 7, 256, 256], P(None, None, ('gx', 'gy')), may hold values from -6 to 6, as said below
Outputs:
- magnet_next: float32 [3, 4, 256, 256], P(None, None, ('run', 'gx', 'gy')), parts along dimension 2
- effective_field: float32 [3, 4, 256, 256], P(None, None, ('run', 'gx', 'gy')), parts along dimension 2
The draws below stay inside these ranges and needn't reach their ends.
There are 2 independent parts, one for each index of `run`. The reference program is written for one: setup_inputs(seed, part) draws one part's arguments, and reference() takes and returns one part's arrays. A program takes and returns all parts, laid end to end along the dimension named above; an argument that names none is the same for every part. Nothing has to cross between parts.
Inputs may be any that keep to these rules, and one draw needn't show every extreme that they name: `magnet`: each cell's three components form a unit vector. kernel[c, d, ky, kx] equals t_c kernel[c, d, ky, (256 - kx) mod 256] with t_c = -1 for c = 3 and 4, 1 otherwise; it equals u_c kernel[c, 6 - d, ky, kx] with u_c = -1 for c = 4 and 5, 1 otherwise; components 3 and 5 are zero at ky = 0.
All inputs are finite; a program needn't handle non-finite values. No bound on the sum of `region` on one device may be relied on, other than what follows from the above.
Results may differ from the reference program's by a relative error of at most 0.0001.
Values sent between devices are 32-bit elements; how exact they have to be, the bound alone decides.
No kernel may reach another device: no remote copies, remote signals or barrier semaphores. Data moves between devices by JAX's collectives and lax.ppermute only.
A program may use at most 128 MiB of HBM per device.

```python
import math
import jax
import jax.numpy as jnp
import numpy as np
from jax import lax

CX = 8
NY = 256
NZ = 4
NX = 128
KX = 256
KY = 511
DZ = 7


def draw_magnet(key, part):
    key_height, key_angle = jax.random.split(key)
    shape = (NZ, NX, NY)
    height = jax.random.uniform(key_height, shape, jnp.float32, -0.98, 0.98)
    angles = jax.random.uniform(key_angle, shape, jnp.float32, -math.pi, math.pi)
    radial = jnp.sqrt(1.0 - height * height)
    return jnp.stack([radial * jnp.cos(angles), radial * jnp.sin(angles), height]).astype(jnp.float32)


def draw_kernel(key, part):
    shape = (6, DZ, NY, KX)
    sample = jnp.clip(2.0 * jax.random.normal(key, shape, jnp.float32), -6.0, 6.0)
    track_sign = jnp.array([1.0, 1.0, 1.0, -1.0, -1.0, 1.0], jnp.float32).reshape(6, 1, 1, 1)
    layer_sign = jnp.array([1.0, 1.0, 1.0, 1.0, -1.0, -1.0], jnp.float32).reshape(6, 1, 1, 1)
    width_sign = jnp.array([1.0, 1.0, 1.0, -1.0, 1.0, -1.0], jnp.float32).reshape(6, 1, 1, 1)
    flipped = jnp.roll(jnp.flip(sample, 3), 1, 3)
    even_track = 0.5 * (sample + track_sign * flipped)
    parity = 0.5 * (even_track + layer_sign * jnp.flip(even_track, 1))
    kept_rows = (width_sign > 0.0) | (jnp.arange(NY) > 0)[None, None, :, None]
    return jnp.where(kept_rows, parity, 0.0).astype(jnp.float32)


def with_ends(result, rng, smallest, high):
    longest = result.shape.index(max(result.shape))
    spots = []
    for shift in (0, 1):
        where = [jax.random.randint(jax.random.fold_in(rng, axis), (), 0, length) for axis, length in enumerate(result.shape)]
        where[longest] = (where[longest] + shift) % result.shape[longest]
        spots.append(tuple(where))
    return result.at[spots[0]].set(smallest).at[spots[1]].set(high)


def setup_inputs(seed: int = 0, part: int = 0) -> dict:
    streams_of = jax.random.split(jax.random.key(seed), 6)
    own_keys = jax.random.split(jax.random.fold_in(streams_of[5], part), 6)
    return {
        "magnet": draw_magnet(jax.random.fold_in(jax.random.fold_in(streams_of[5], part), 71), part),
        "window_shift": jax.random.randint(own_keys[1], (1,), 1, CX).astype(jnp.int32),
        "region": with_ends((jax.random.randint(own_keys[2], (NX, NY), 0, 4) < 3).astype(jnp.int32), jax.random.fold_in(own_keys[2], 1), 0, 1),
        "material": jnp.clip(jnp.exp(jax.random.uniform(streams_of[3], (NZ, 5), jnp.float32, math.log(0.1), math.log(1.0))), 0.1, 1.0),
        "kernel": draw_kernel(jax.random.fold_in(streams_of[5], 71), part),
    }


time_step = 0.1
pair_comp = ((0, 3, 4), (3, 1, 5), (4, 5, 2))


def cross_product(left, right):
    return jnp.stack([left[1] * right[2] - left[2] * right[1],
                      left[2] * right[0] - left[0] * right[2],
                      left[0] * right[1] - left[1] * right[0]])


def neighbours(state):
    padded = jnp.pad(state, ((0, 0), (1, 1), (1, 1), (1, 1)), mode="edge")
    laplace = padded[:, 2:, 1:-1, 1:-1] + padded[:, :-2, 1:-1, 1:-1]
    laplace = laplace + padded[:, 1:-1, 2:, 1:-1] + padded[:, 1:-1, :-2, 1:-1]
    laplace = laplace + padded[:, 1:-1, 1:-1, 2:] + padded[:, 1:-1, 1:-1, :-2] - 6.0 * state
    slope = 0.5 * (padded[:, 1:-1, 2:, 1:-1] - padded[:, 1:-1, :-2, 1:-1])
    return laplace, slope


def demag_field(state, kernel_full):
    dz_table = np.arange(NZ)[:, None] - np.arange(NZ)[None, :] + NZ - 1
    turned = jnp.transpose(state, (0, 1, 3, 2))
    spectrum = jnp.fft.fft2(turned, s=(KY, KX), axes=(2, 3))
    real_in = jnp.real(spectrum)
    imag_in = jnp.imag(spectrum)
    comps = []
    for i in range(3):
        real_sum = jnp.zeros((NZ, KY, KX), jnp.float32)
        imag_sum = jnp.zeros((NZ, KY, KX), jnp.float32)
        for j in range(3):
            index_c = pair_comp[i][j]
            pairs = kernel_full[index_c][dz_table]
            real_term = jnp.einsum("zwab,wab->zab", pairs, real_in[j], precision=lax.Precision.HIGHEST)
            imag_term = jnp.einsum("zwab,wab->zab", pairs, imag_in[j], precision=lax.Precision.HIGHEST)
            if index_c >= 4:
                real_sum = real_sum - imag_term
                imag_sum = imag_sum + real_term
            else:
                real_sum = real_sum + real_term
                imag_sum = imag_sum + imag_term
        inverse = jnp.fft.ifft2(lax.complex(real_sum, imag_sum), axes=(1, 2))
        comps.append(jnp.real(inverse)[:, :NY, :NX])
    return jnp.transpose(jnp.stack(comps), (0, 1, 3, 2))


def reference(magnet, window_shift, region, material, kernel):
    width_sign = jnp.array([1.0, 1.0, 1.0, -1.0, 1.0, -1.0], jnp.float32).reshape(6, 1, 1, 1)
    mirrored = width_sign * jnp.flip(kernel[:, :, 1:], axis=2)
    kernel_full = jnp.concatenate([kernel, mirrored], axis=2)
    offset = window_shift[0]
    padded = jnp.concatenate([magnet, jnp.zeros((3, NZ, CX, NY), jnp.float32)], axis=2)
    moved = lax.dynamic_slice_in_dim(padded, offset, NX, 2)
    cells = jnp.arange(NX, dtype=jnp.int32)
    fill_up = (jnp.arange(3) == 2).astype(jnp.float32).reshape(3, 1, 1, 1)
    window = jnp.where((cells >= NX - offset)[None, None, :, None], fill_up, moved)
    damping = material[:, 0].reshape(1, NZ, 1, 1)
    nonadiabatic = material[:, 1].reshape(1, NZ, 1, 1)
    stiffness = material[:, 2].reshape(1, NZ, 1, 1)
    anisotropy = material[:, 3].reshape(1, NZ, 1, 1)
    drift_speed = material[:, 4].reshape(1, NZ, 1, 1) * region.astype(jnp.float32)[None, None]

    def rate_of(state):
        laplace, slope = neighbours(state)
        effective = stiffness * laplace + anisotropy * state[2:3] * fill_up + demag_field(state, kernel_full)
        drift_term = drift_speed * slope
        torque_h = cross_product(state, effective)
        damping_h = cross_product(state, torque_h)
        torque_u = cross_product(state, drift_term)
        damping_u = cross_product(state, torque_u)
        change = (-torque_h - damping * damping_h + (1.0 + damping * nonadiabatic) * damping_u
                  + (nonadiabatic - damping) * torque_u) / (1.0 + damping * damping)
        return change, effective

    section_one, effective_field = rate_of(window)
    section_two, _ = rate_of(window + 0.5 * time_step * section_one)
    section_three, _ = rate_of(window + 0.5 * time_step * section_two)
    section_four, _ = rate_of(window + time_step * section_three)
    magnet_next = window + (time_step / 6.0) * (section_one + 2.0 * section_two + 2.0 * section_three + section_four)
    return magnet_next, effective_field
```

```python
import functools
import math

import jax
import jax.numpy as jnp
import numpy as np
from jax import lax
from jax.experimental import pallas as pl
from jax.experimental.pallas import tpu as pltpu
from jax.sharding import PartitionSpec as P

time_step = 0.1
pair_comp = ((0, 3, 4), (3, 1, 5), (4, 5, 2))
highest = lax.Precision.HIGHEST
lanes = 128


def passed_along(value, axis, steps):
    count = lax.axis_size(axis)
    leading, last = (max(0, -steps), min(count, count - steps))
    return lax.ppermute(value, axis, [(source, source + steps) for source in range(leading, last)])


def with_halo(cells, sides, width):
    for axis, dim in sides:
        count = lax.axis_size(axis)
        ends = count - 1
        head = lax.slice_in_dim(cells, 0, width, axis=dim)
        tail = lax.slice_in_dim(cells, cells.shape[dim] - width, cells.shape[dim], axis=dim)
        cells = jnp.concatenate(
            [
                lax.ppermute(tail, axis, [(i, (i + 1) % count) for i in range(ends)]),
                cells,
                lax.ppermute(head, axis, [((i + 1) % count, i) for i in range(ends)]),
            ],
            axis=dim,
        )
    return cells


def cross_product(left, right):
    return jnp.stack(
        [
            left[1] * right[2] - left[2] * right[1],
            left[2] * right[0] - left[0] * right[2],
            left[0] * right[1] - left[1] * right[0],
        ]
    )


def phases(count_rows, count_cols, length, direction):
    product = (
        jnp.arange(count_rows, dtype=jnp.int32)[:, None]
        * jnp.arange(count_cols, dtype=jnp.int32)[None, :]
        % length
    )
    angles = direction * 2.0 * math.pi / length * product.astype(jnp.float32)
    return (jnp.cos(angles), jnp.sin(angles))


def complex_table(cosine, sine):
    top_rows = jnp.stack([cosine, sine], axis=1)
    bottom_rows = jnp.stack([-sine, cosine], axis=1)
    return jnp.stack([top_rows, bottom_rows], axis=0)


def twist(first_pass, cosine, sine):
    real_part = first_pass[:, 0]
    imag_part = first_pass[:, 1]
    return jnp.stack(
        [real_part * cosine - imag_part * sine, real_part * sine + imag_part * cosine], axis=1
    )


def forward_track(values):
    batch, pair, track_cells = values.shape
    track_freq = 2 * track_cells
    outer_len = track_freq // 64
    outer_used = track_cells // 64
    blocked = values.reshape(batch, 2, outer_used, 64)
    cosine, sine = phases(outer_used, outer_len, outer_len, -1.0)
    first_pass = jnp.einsum(
        "bpxa,pxqk->bqka", blocked, complex_table(cosine, sine), precision=highest
    )
    twist_cos, twist_sin = phases(outer_len, 64, track_freq, -1.0)
    twisted = twist(first_pass, twist_cos, twist_sin)
    cosine, sine = phases(64, 64, 64, -1.0)
    result = jnp.einsum("bpka,paqj->bqjk", twisted, complex_table(cosine, sine), precision=highest)
    return result.reshape(batch, 2, track_freq)


def inverse_track(values):
    batch, pair, track_freq = values.shape
    track_cells = track_freq // 2
    outer_len = track_freq // 64
    outer_used = track_cells // 64
    blocked = values.reshape(batch, 2, 64, outer_len)
    cosine, sine = phases(64, 64, 64, 1.0)
    first_pass = jnp.einsum(
        "bpjk,pjqa->bqka", blocked, complex_table(cosine, sine), precision=highest
    )
    twist_cos, twist_sin = phases(outer_len, 64, track_freq, 1.0)
    twisted = twist(first_pass, twist_cos, twist_sin)
    cosine, sine = phases(outer_len, outer_used, outer_len, 1.0)
    result = jnp.einsum("bpka,pkqx->bqxa", twisted, complex_table(cosine, sine), precision=highest)
    return result.reshape(batch, 2, track_cells)


def apply_kernel(spectrum, kernel_pairs):
    fields = []
    for i in range(3):
        summed = None
        for j in range(3):
            index_c = pair_comp[i][j]
            table = kernel_pairs[index_c][:, :, :, None, :]
            contrib = jnp.sum(table * spectrum[j][None], axis=1)
            if index_c >= 4:
                contrib = jnp.stack([-contrib[:, :, 1], contrib[:, :, 0]], axis=2)
            summed = contrib if summed is None else summed + contrib
        fields.append(summed)
    return jnp.stack(fields)


def clamp_ends(widened, position, devices):
    head_row = jnp.where(position == 0, widened[:, :, 1:2], widened[:, :, 0:1])
    tail_row = jnp.where(position == devices - 1, widened[:, :, -2:-1], widened[:, :, -1:])
    return jnp.concatenate([head_row, widened[:, :, 1:-1], tail_row], axis=2)


def demag_field(state, kernel_pairs, forward_y, inverse_y):
    components, layers, slab_rows, width_cells = state.shape
    devices = lax.axis_size(("gx", "gy"))
    local_freq = width_cells // devices
    track_cells = slab_rows * devices
    track_freq = 2 * track_cells
    spectrum = jnp.einsum("czxy,ypk->czkpx", state, forward_y, precision=highest)
    blocks = spectrum.reshape(components, layers, devices, local_freq, 2, 1, slab_rows)
    arrived = lax.all_to_all(blocks, ("gx", "gy"), split_axis=2, concat_axis=5, tiled=True)
    flat_rows = arrived.reshape(components * layers * local_freq, 2, track_cells)
    spectrum_x = forward_track(flat_rows).reshape(components, layers, local_freq, 2, track_freq)
    product_hat = apply_kernel(spectrum_x, kernel_pairs)
    returned_x = inverse_track(product_hat.reshape(components * layers * local_freq, 2, track_freq))
    pieces = returned_x.reshape(components, layers, 1, local_freq, 2, devices, slab_rows)
    landed = lax.all_to_all(pieces, ("gx", "gy"), split_axis=5, concat_axis=2, tiled=True)
    gathered_y = landed.reshape(components, layers, width_cells, 2, slab_rows)
    return jnp.einsum("czkpx,kpy->czxy", gathered_y, inverse_y, precision=highest)


def local(magnet, window_shift, region, material, kernel):
    components, layers, slab_rows, width_cells = magnet.shape
    devices = lax.axis_size(("gx", "gy"))
    position = lax.axis_index(("gx", "gy"))
    track_cells = slab_rows * devices
    track_freq = 2 * track_cells
    freq_len = 2 * width_cells - 1
    offset = window_shift[0]
    fill_up = (jnp.arange(3) == 2).astype(jnp.float32).reshape(3, 1, 1, 1)
    following = passed_along(magnet, ("gx", "gy"), -1)
    joined = jnp.concatenate([magnet, following], axis=2)
    widened = lax.dynamic_slice_in_dim(joined, offset - 1, slab_rows + 2, 2)
    global_cell = position * slab_rows - 1 + jnp.arange(slab_rows + 2, dtype=jnp.int32)
    widened = jnp.where(
        (global_cell >= track_cells - offset)[None, None, :, None], fill_up, widened
    )
    initial = widened[:, :, 1:-1]
    first_widened = clamp_ends(widened, position, devices)
    dz_table = np.arange(layers)[:, None] - np.arange(layers)[None, :] + layers - 1
    kernel_pairs = kernel[:, dz_table]
    cosine, sine = phases(width_cells, width_cells, freq_len, -1.0)
    forward_y = jnp.stack([cosine, sine], axis=1)
    cosine, sine = phases(width_cells, width_cells, freq_len, 1.0)
    weight = jnp.where(jnp.arange(width_cells) == 0, 1.0, 2.0).astype(jnp.float32)[:, None]
    inverse_y = jnp.stack([weight * cosine, -weight * sine], axis=1) / float(track_freq * freq_len)
    damping = material[:, 0].reshape(1, layers, 1, 1)
    nonadiabatic = material[:, 1].reshape(1, layers, 1, 1)
    stiffness = material[:, 2].reshape(1, layers, 1, 1)
    anisotropy = material[:, 3].reshape(1, layers, 1, 1)
    drift_speed = material[:, 4].reshape(1, layers, 1, 1) * region.astype(jnp.float32)[None, None]

    def rate_of(state, widened_in):
        if widened_in is None:
            widened_in = clamp_ends(with_halo(state, ((("gx", "gy"), 2),), 1), position, devices)
        width_pad = jnp.pad(state, ((0, 0), (0, 0), (0, 0), (1, 1)), mode="edge")
        layer_pad = jnp.pad(state, ((0, 0), (1, 1), (0, 0), (0, 0)), mode="edge")
        laplace = widened_in[:, :, 2:] + widened_in[:, :, :-2]
        laplace = laplace + width_pad[:, :, :, 2:] + width_pad[:, :, :, :-2]
        laplace = laplace + layer_pad[:, 2:] + layer_pad[:, :-2] - 6.0 * state
        slope = 0.5 * (widened_in[:, :, 2:] - widened_in[:, :, :-2])
        effective = stiffness * laplace + anisotropy * state[2:3] * fill_up
        effective = effective + demag_field(state, kernel_pairs, forward_y, inverse_y)
        drift_term = drift_speed * slope
        torque_h = cross_product(state, effective)
        damping_h = cross_product(state, torque_h)
        torque_u = cross_product(state, drift_term)
        damping_u = cross_product(state, torque_u)
        change = (
            -torque_h
            - damping * damping_h
            + (1.0 + damping * nonadiabatic) * damping_u
            + (nonadiabatic - damping) * torque_u
        ) / (1.0 + damping * damping)
        return (change, effective)

    section_one, effective_field = rate_of(initial, first_widened)
    section_two, _ = rate_of(initial + 0.5 * time_step * section_one, None)
    section_three, _ = rate_of(initial + 0.5 * time_step * section_two, None)
    section_four, _ = rate_of(initial + time_step * section_three, None)
    magnet_next = initial + time_step / 6.0 * (
        section_one + 2.0 * section_two + 2.0 * section_three + section_four
    )
    return (magnet_next, effective_field)


def split_table(table):
    table = np.asarray(table, np.float64).astype(np.float32)
    high = table.astype(jnp.bfloat16)
    low = (table - high.astype(np.float32)).astype(jnp.bfloat16)
    return (high, low)


def angle_table(rows, cols, length):
    product = np.outer(np.arange(rows), np.arange(cols)) % length
    return 2.0 * np.pi / length * product


def width_tables(width_cells, devices, scale):
    freq_len = 2 * width_cells - 1
    angles = angle_table(width_cells, width_cells, freq_len)
    shape = (width_cells, devices, 1, width_cells // devices)
    cosine, sine = np.cos(angles).reshape(shape), np.sin(angles).reshape(shape)
    forward = np.concatenate([cosine, -sine], axis=2).reshape(width_cells, 2 * width_cells)
    weight = np.where(np.arange(width_cells) == 0, 1.0, 2.0).reshape(shape[1:]) * scale
    inverse = np.concatenate([weight * cosine, -weight * sine], axis=2)
    return (forward, inverse.reshape(width_cells, 2 * width_cells).T)


def track_tables(track_cells):
    angles = angle_table(track_cells, track_cells, 2 * track_cells)
    cosine, sine = np.cos(angles), np.sin(angles)
    sine[:, 0] = np.where(np.arange(track_cells) % 2 == 0, 1.0, -1.0)
    weight = np.where(np.arange(track_cells) == 0, 1.0, 2.0)
    forward = np.concatenate([cosine, sine], axis=1)
    inverse = np.concatenate([weight * cosine, weight * sine], axis=1)
    return (forward, inverse)


def halves(value):
    high = value.astype(jnp.bfloat16)
    return (high, (value - high.astype(jnp.float32)).astype(jnp.bfloat16))


def dot_halves(left, right, dims=((1,), (0,))):
    def dot(a, b):
        return lax.dot_general(a, b, (dims, ((), ())), preferred_element_type=jnp.float32)

    return dot(left[0], right[0]) + (dot(left[0], right[1]) + dot(left[1], right[0]))


def turn_blocks(blocks, size):
    count = len(blocks)
    group = lax.broadcasted_iota(jnp.int32, blocks[0].shape, 1) // size
    results = []
    for j in range(count):
        result = None
        for i in range(count):
            shift = (i - j) * size % (count * size)
            moved = pltpu.roll(blocks[i], shift, 1) if shift else blocks[i]
            result = moved if result is None else jnp.where(group == i, moved, result)
        results.append(result)
    return results


def send_forward(cells, forward_refs, send_ref, devices):
    slab_rows = send_ref.shape[1]
    size = 2 * forward_refs[0].shape[0] // devices
    per_tile = lanes // size
    spectrum = dot_halves(halves(cells), (forward_refs[0][...], forward_refs[1][...]))
    fields = cells.shape[0] // slab_rows
    for a in range(fields // per_tile):
        for q in range(devices // per_tile):
            blocks = [
                spectrum[(a * per_tile + b) * slab_rows : (a * per_tile + b + 1) * slab_rows, q * lanes : (q + 1) * lanes]
                for b in range(per_tile)
            ]
            for b, block in enumerate(turn_blocks(blocks, size)):
                send_ref[q * per_tile + b, :, a * lanes : (a + 1) * lanes] = block


def take_inverse(received_ref, inverse_refs, rows_ref):
    devices, slab_rows, width = received_ref.shape
    size = inverse_refs[0].shape[0] // devices
    per_tile = lanes // size
    fields = width // size
    for a in range(fields // per_tile):
        for q in range(devices // per_tile):
            blocks = [
                received_ref[q * per_tile + b, :, a * lanes : (a + 1) * lanes] for b in range(per_tile)
            ]
            for b, block in enumerate(turn_blocks(blocks, size)):
                row = (a * per_tile + b) * slab_rows
                rows_ref[row : row + slab_rows, q * lanes : (q + 1) * lanes] = block
    return dot_halves(halves(rows_ref[...]), (inverse_refs[0][...], inverse_refs[1][...]))


def window_kernel(devices, place_ref, magnet_ref, following_ref, *refs):
    forward_refs = refs[:2]
    initial_ref, before_ref, after_ref, send_ref, joined_ref, moved_ref = refs[2:]
    components, layers, slab_rows, width = magnet_ref.shape
    fields = components * layers
    position = place_ref[0]
    offset = place_ref[1]
    limit = devices * slab_rows - offset - position * slab_rows
    joined_ref[:, 0:slab_rows, :] = magnet_ref[...].reshape(fields, slab_rows, width)
    joined_ref[:, slab_rows : 2 * slab_rows, :] = following_ref[...].reshape(fields, slab_rows, width)

    for choice in range(1, slab_rows):

        @pl.when(offset == choice)
        def move():
            for f in range(fields):
                moved_ref[f] = joined_ref[f, choice : choice + slab_rows, :]
                before_ref[f : f + 1, :] = joined_ref[f, choice - 1 : choice, :]
                after_ref[f : f + 1, :] = joined_ref[f, choice + slab_rows : choice + slab_rows + 1, :]

    def filled(rows, cell, field):
        return jnp.where(cell >= limit, jnp.where(field >= fields - layers, 1.0, 0.0), rows)

    rows = moved_ref[...]
    cell = lax.broadcasted_iota(jnp.int32, rows.shape, 1)
    state = filled(rows, cell, lax.broadcasted_iota(jnp.int32, rows.shape, 0))
    edge = lax.broadcasted_iota(jnp.int32, (fields, width), 0)
    before_ref[...] = filled(before_ref[...], jnp.full((fields, width), -1, jnp.int32), edge)
    after_ref[...] = filled(after_ref[...], jnp.full((fields, width), slab_rows, jnp.int32), edge)
    initial_ref[...] = state.reshape(components, layers, slab_rows, width)
    send_forward(state.reshape(fields * slab_rows, width), forward_refs, send_ref, devices)


def track_kernel(received_ref, table_ref, wf_high, wf_low, wi_high, wi_low, send_ref, spectrum_ref, product_ref):
    devices, slab_rows, width = received_ref.shape
    components = 3
    layers, local_freq = table_ref.shape[1:3]
    track = devices * slab_rows
    flat = received_ref[...].reshape(track, width).T
    spectrum_ref[...] = dot_halves(halves(flat), (wf_high[...], wf_low[...]))
    step = 8
    first_lane = lax.broadcasted_iota(jnp.int32, (step, track), 1) == 0
    for start in range(0, local_freq, step):

        def part(j, w, p, half):
            row = ((j * layers + w) * 2 + p) * local_freq + start
            return (slice(row, row + step), slice(half * track, (half + 1) * track))

        tables = {}
        for c in range(6):
            for e in range(layers):
                cosine = table_ref[c, e, start : start + step, 0:track]
                nyquist = table_ref[c, e, start : start + step, track : 2 * track]
                tables[c, e] = (cosine, jnp.where(first_lane, nyquist, cosine) if c in (0, 1, 2, 5) else cosine)
        for i in range(components):
            for z in range(layers):
                sums = [None] * 4

                def add(slot, value, sign):
                    if sums[slot] is None:
                        sums[slot] = value if sign > 0 else -value
                    else:
                        sums[slot] = sums[slot] + value if sign > 0 else sums[slot] - value

                for j in range(components):
                    c = pair_comp[i][j]
                    for w in range(layers):
                        even, odd = tables[c, abs(z - w)]
                        sign = -1 if z < w and c >= 4 else 1
                        ac, as_, bc, bs = [
                            spectrum_ref[part(j, w, p, half)] for p in range(2) for half in range(2)
                        ]
                        if c <= 2:
                            terms = ((even * ac, 1), (odd * as_, 1), (even * bc, 1), (odd * bs, 1))
                        elif c == 3:
                            terms = ((even * bs, 1), (even * bc, -1), (even * as_, -1), (even * ac, 1))
                        elif c == 4:
                            terms = ((even * as_, 1), (even * ac, -1), (even * bs, 1), (even * bc, -1))
                        else:
                            terms = ((even * bc, -1), (odd * bs, -1), (even * ac, 1), (odd * as_, 1))
                        for slot, (value, term_sign) in enumerate(terms):
                            add(slot, value, term_sign * sign)
                for slot in range(4):
                    product_ref[part(i, z, slot // 2, slot % 2)] = sums[slot]
    result = dot_halves((wi_high[...], wi_low[...]), halves(product_ref[...]), ((1,), (1,)))
    send_ref[...] = result.reshape(devices, slab_rows, width)


def step_kernel(stage, devices, place_ref, coef_ref, received_ref, state_ref, before_ref, after_ref, region_ref, *refs):
    refs = list(refs)
    inverse_refs = [refs.pop(0), refs.pop(0)]
    forward_refs = [refs.pop(0), refs.pop(0)] if stage < 3 else None
    initial_ref = refs.pop(0) if stage > 0 else state_ref
    sum_ref = refs.pop(0) if stage > 0 else None
    field_ref = refs.pop(0) if stage == 0 else None
    next_ref = refs.pop(0)
    if stage < 3:
        total_ref, head_ref, tail_ref, send_ref = [refs.pop(0) for _ in range(4)]
    rows_ref = refs.pop(0)
    components, layers, slab_rows, width = state_ref.shape
    position = place_ref[0]
    demag = take_inverse(received_ref, inverse_refs, rows_ref)
    shape = (slab_rows, width)
    row = lax.broadcasted_iota(jnp.int32, shape, 0)
    col = lax.broadcasted_iota(jnp.int32, shape, 1)
    flow = region_ref[...].astype(jnp.float32)
    is_first = (position == 0).astype(jnp.int32)
    is_last = (position == devices - 1).astype(jnp.int32)
    fields = []
    moved = []
    for z in range(layers):
        stiffness, anisotropy, drift = (coef_ref[z, 4], coef_ref[z, 5], coef_ref[z, 6])
        m, h, g = ([], [], [])
        for c in range(components):
            f = c * layers + z
            cells = state_ref[c, z]
            head = jnp.where(is_first == 1, cells[0:1], before_ref[f : f + 1, :])
            tail = jnp.where(is_last == 1, cells[slab_rows - 1 : slab_rows], after_ref[f : f + 1, :])
            lower = jnp.where(row == 0, head, pltpu.roll(cells, 1, 0))
            upper = jnp.where(row == slab_rows - 1, tail, pltpu.roll(cells, slab_rows - 1, 0))
            left = jnp.where(col == 0, cells, pltpu.roll(cells, 1, 1))
            right = jnp.where(col == width - 1, cells, pltpu.roll(cells, width - 1, 1))
            laplace = (upper + lower) + (left + right)
            laplace = laplace + state_ref[c, max(z - 1, 0)] + state_ref[c, min(z + 1, layers - 1)] - 6.0 * cells
            effective = stiffness * laplace + demag[f * slab_rows : (f + 1) * slab_rows, :]
            if c == 2:
                effective = effective + anisotropy * cells
            if stage == 0:
                field_ref[c, z] = effective
            m.append(cells)
            h.append(effective)
            g.append((0.5 * drift) * flow * (upper - lower))
        inner = [coef_ref[z, 1] * h[c] + coef_ref[z, 2] * g[c] for c in range(3)]
        outer = [coef_ref[z, 0] * h[c] + coef_ref[z, 3] * g[c] for c in range(3)]
        turned = [m[(c + 1) % 3] * inner[(c + 2) % 3] - m[(c + 2) % 3] * inner[(c + 1) % 3] for c in range(3)]
        whole = [outer[c] + turned[c] for c in range(3)]
        for c in range(components):
            rate = m[(c + 1) % 3] * whole[(c + 2) % 3] - m[(c + 2) % 3] * whole[(c + 1) % 3]
            start = initial_ref[c, z]
            if stage == 3:
                next_ref[c, z] = start + (time_step / 6.0) * (sum_ref[c, z] + rate)
            else:
                factor = time_step if stage == 2 else 0.5 * time_step
                value = start + factor * rate
                next_ref[c, z] = value
                f = c * layers + z
                head_ref[f : f + 1, :] = value[0:1]
                tail_ref[f : f + 1, :] = value[slab_rows - 1 : slab_rows]
                total_ref[c, z] = rate if stage == 0 else sum_ref[c, z] + 2.0 * rate
    if stage < 3:
        cells = next_ref[...].reshape(components * layers * slab_rows, width)
        send_forward(cells, forward_refs, send_ref, devices)


def call(body, name, outs, in_smem, args, scratch):
    in_specs = [
        pl.BlockSpec(memory_space=pltpu.SMEM if i < in_smem else pltpu.VMEM) for i in range(len(args))
    ]
    return pl.pallas_call(
        body,
        name=name,
        out_shape=[jax.ShapeDtypeStruct(s, jnp.float32) for s in outs],
        in_specs=in_specs,
        out_specs=[pl.BlockSpec(memory_space=pltpu.VMEM) for _ in outs],
        scratch_shapes=[pltpu.VMEM(s, jnp.float32) for s in scratch],
        compiler_params=pltpu.CompilerParams(vmem_limit_bytes=24 * 1024 * 1024),
    )(*args)


def exchange(blocks):
    return lax.all_to_all(blocks, ("gx", "gy"), split_axis=0, concat_axis=0, tiled=True)


def local_tiled(magnet, window_shift, region, material, kernel):
    components, layers, slab_rows, width = magnet.shape
    devices = lax.axis_size(("gx", "gy"))
    position = lax.axis_index(("gx", "gy"))
    track = slab_rows * devices
    fields = components * layers
    scale = 1.0 / (2 * track * (2 * width - 1))
    forward, inverse = [split_table(t) for t in width_tables(width, devices, scale)]
    track_forward, track_inverse = [split_table(t) for t in track_tables(track)]
    row_width = 2 * fields * (width // devices)
    block_shape = (devices, slab_rows, row_width)
    following = passed_along(magnet, ("gx", "gy"), -1)
    place = jnp.stack([position.astype(jnp.int32), window_shift[0]])
    a, b = (material[:, 0], material[:, 1])
    below = 1.0 / (1.0 + a * a)
    zero = jnp.zeros_like(a)
    coef = jnp.stack(
        [-below, -a * below, (1.0 + a * b) * below, (b - a) * below, material[:, 2], material[:, 3], material[:, 4], zero],
        axis=1,
    )
    table = kernel[:, layers - 1 :]
    initial, before, after, send = call(
        functools.partial(window_kernel, devices),
        "window",
        [magnet.shape, (fields, width), (fields, width), block_shape],
        1,
        [place, magnet, following, *forward],
        [(fields, 2 * slab_rows, width), (fields, slab_rows, width)],
    )
    state = initial
    total = None
    for stage in range(4):
        received = exchange(send)
        (back,) = call(
            track_kernel,
            "track",
            [block_shape],
            0,
            [received, table, *track_forward, *track_inverse],
            [(row_width, 2 * track), (row_width, 2 * track)],
        )
        returned = exchange(back)
        args = [place, coef, returned, state, before, after, region, *inverse]
        outs = [magnet.shape]
        if stage < 3:
            args += [*forward]
            outs += [magnet.shape, (fields, width), (fields, width), block_shape]
        if stage > 0:
            args += [initial, total]
        else:
            outs = [magnet.shape] + outs
        results = list(
            call(
                functools.partial(step_kernel, stage, devices),
                "step",
                outs,
                2,
                args,
                [(fields * slab_rows, 2 * width)],
            )
        )
        if stage == 0:
            effective_field = results.pop(0)
        state = results.pop(0)
        if stage < 3:
            total, head, tail, send = results
            before = passed_along(tail, ("gx", "gy"), 1)
            after = passed_along(head, ("gx", "gy"), -1)
    return (state, effective_field)


def fits_tiles(mesh_devices, width):
    size = 2 * (width // mesh_devices)
    return size % 16 == 0 and lanes % size == 0 and mesh_devices % (lanes // size) == 0


def local_any(magnet, window_shift, region, material, kernel):
    components, layers, slab_rows, width = magnet.shape
    devices = lax.axis_size(("gx", "gy"))
    track = slab_rows * devices
    per_tile = lanes * devices // (2 * width)
    tiled = fits_tiles(devices, width) and slab_rows % 8 == 0 and track % lanes == 0 and width % lanes == 0
    tiled = tiled and components * layers % max(per_tile, 1) == 0
    return (local_tiled if tiled else local)(magnet, window_shift, region, material, kernel)


def solution(mesh):
    in_specs = (
        P(None, None, ("run", "gx", "gy"), None),
        P("run"),
        P(("run", "gx", "gy"), None),
        P(),
        P(None, None, ("gx", "gy"), None),
    )
    out_specs = (P(None, None, ("run", "gx", "gy"), None), P(None, None, ("run", "gx", "gy"), None))
    return jax.shard_map(local_any, mesh=mesh, in_specs=in_specs, out_specs=out_specs, check_vma=False)
```

```python
import functools
import math

import jax
import jax.numpy as jnp
import numpy as np
from jax import lax
from jax.experimental import pallas as pl
from jax.experimental.pallas import tpu as pltpu
from jax.sharding import PartitionSpec as P

time_step = 0.1
pair_comp = ((0, 3, 4), (3, 1, 5), (4, 5, 2))
highest = lax.Precision.HIGHEST
lanes = 128


def passed_along(value, axis, steps):
    count = lax.axis_size(axis)
    leading, last = (max(0, -steps), min(count, count - steps))
    return lax.ppermute(value, axis, [(source, source + steps) for source in range(leading, last)])


def with_halo(cells, sides, width):
    for axis, dim in sides:
        count = lax.axis_size(axis)
        ends = count - 1
        head = lax.slice_in_dim(cells, 0, width, axis=dim)
        tail = lax.slice_in_dim(cells, cells.shape[dim] - width, cells.shape[dim], axis=dim)
        cells = jnp.concatenate(
            [
                lax.ppermute(tail, axis, [(i, (i + 1) % count) for i in range(ends)]),
                cells,
                lax.ppermute(head, axis, [((i + 1) % count, i) for i in range(ends)]),
            ],
            axis=dim,
        )
    return cells


def cross_product(left, right):
    return jnp.stack(
        [
            left[1] * right[2] - left[2] * right[1],
            left[2] * right[0] - left[0] * right[2],
            left[0] * right[1] - left[1] * right[0],
        ]
    )


def phases(count_rows, count_cols, length, direction):
    product = (
        jnp.arange(count_rows, dtype=jnp.int32)[:, None]
        * jnp.arange(count_cols, dtype=jnp.int32)[None, :]
        % length
    )
    angles = direction * 2.0 * math.pi / length * product.astype(jnp.float32)
    return (jnp.cos(angles), jnp.sin(angles))


def complex_table(cosine, sine):
    top_rows = jnp.stack([cosine, sine], axis=1)
    bottom_rows = jnp.stack([-sine, cosine], axis=1)
    return jnp.stack([top_rows, bottom_rows], axis=0)


def twist(first_pass, cosine, sine):
    real_part = first_pass[:, 0]
    imag_part = first_pass[:, 1]
    return jnp.stack(
        [real_part * cosine - imag_part * sine, real_part * sine + imag_part * cosine], axis=1
    )


def forward_track(values):
    batch, pair, track_cells = values.shape
    track_freq = 2 * track_cells
    outer_len = track_freq // 64
    outer_used = track_cells // 64
    blocked = values.reshape(batch, 2, outer_used, 64)
    cosine, sine = phases(outer_used, outer_len, outer_len, -1.0)
    first_pass = jnp.einsum(
        "bpxa,pxqk->bqka", blocked, complex_table(cosine, sine), precision=highest
    )
    twist_cos, twist_sin = phases(outer_len, 64, track_freq, -1.0)
    twisted = twist(first_pass, twist_cos, twist_sin)
    cosine, sine = phases(64, 64, 64, -1.0)
    result = jnp.einsum("bpka,paqj->bqjk", twisted, complex_table(cosine, sine), precision=highest)
    return result.reshape(batch, 2, track_freq)


def inverse_track(values):
    batch, pair, track_freq = values.shape
    track_cells = track_freq // 2
    outer_len = track_freq // 64
    outer_used = track_cells // 64
    blocked = values.reshape(batch, 2, 64, outer_len)
    cosine, sine = phases(64, 64, 64, 1.0)
    first_pass = jnp.einsum(
        "bpjk,pjqa->bqka", blocked, complex_table(cosine, sine), precision=highest
    )
    twist_cos, twist_sin = phases(outer_len, 64, track_freq, 1.0)
    twisted = twist(first_pass, twist_cos, twist_sin)
    cosine, sine = phases(outer_len, outer_used, outer_len, 1.0)
    result = jnp.einsum("bpka,pkqx->bqxa", twisted, complex_table(cosine, sine), precision=highest)
    return result.reshape(batch, 2, track_cells)


def apply_kernel(spectrum, kernel_pairs):
    fields = []
    for i in range(3):
        summed = None
        for j in range(3):
            index_c = pair_comp[i][j]
            table = kernel_pairs[index_c][:, :, :, None, :]
            contrib = jnp.sum(table * spectrum[j][None], axis=1)
            if index_c >= 4:
                contrib = jnp.stack([-contrib[:, :, 1], contrib[:, :, 0]], axis=2)
            summed = contrib if summed is None else summed + contrib
        fields.append(summed)
    return jnp.stack(fields)


def clamp_ends(widened, position, devices):
    head_row = jnp.where(position == 0, widened[:, :, 1:2], widened[:, :, 0:1])
    tail_row = jnp.where(position == devices - 1, widened[:, :, -2:-1], widened[:, :, -1:])
    return jnp.concatenate([head_row, widened[:, :, 1:-1], tail_row], axis=2)


def demag_field(state, kernel_pairs, forward_y, inverse_y):
    components, layers, slab_rows, width_cells = state.shape
    devices = lax.axis_size(("gx", "gy"))
    local_freq = width_cells // devices
    track_cells = slab_rows * devices
    track_freq = 2 * track_cells
    spectrum = jnp.einsum("czxy,ypk->czkpx", state, forward_y, precision=highest)
    blocks = spectrum.reshape(components, layers, devices, local_freq, 2, 1, slab_rows)
    arrived = lax.all_to_all(blocks, ("gx", "gy"), split_axis=2, concat_axis=5, tiled=True)
    flat_rows = arrived.reshape(components * layers * local_freq, 2, track_cells)
    spectrum_x = forward_track(flat_rows).reshape(components, layers, local_freq, 2, track_freq)
    product_hat = apply_kernel(spectrum_x, kernel_pairs)
    returned_x = inverse_track(product_hat.reshape(components * layers * local_freq, 2, track_freq))
    pieces = returned_x.reshape(components, layers, 1, local_freq, 2, devices, slab_rows)
    landed = lax.all_to_all(pieces, ("gx", "gy"), split_axis=5, concat_axis=2, tiled=True)
    gathered_y = landed.reshape(components, layers, width_cells, 2, slab_rows)
    return jnp.einsum("czkpx,kpy->czxy", gathered_y, inverse_y, precision=highest)


def local(magnet, window_shift, region, material, kernel):
    components, layers, slab_rows, width_cells = magnet.shape
    devices = lax.axis_size(("gx", "gy"))
    position = lax.axis_index(("gx", "gy"))
    track_cells = slab_rows * devices
    track_freq = 2 * track_cells
    freq_len = 2 * width_cells - 1
    offset = window_shift[0]
    fill_up = (jnp.arange(3) == 2).astype(jnp.float32).reshape(3, 1, 1, 1)
    following = passed_along(magnet, ("gx", "gy"), -1)
    joined = jnp.concatenate([magnet, following], axis=2)
    widened = lax.dynamic_slice_in_dim(joined, offset - 1, slab_rows + 2, 2)
    global_cell = position * slab_rows - 1 + jnp.arange(slab_rows + 2, dtype=jnp.int32)
    widened = jnp.where(
        (global_cell >= track_cells - offset)[None, None, :, None], fill_up, widened
    )
    initial = widened[:, :, 1:-1]
    first_widened = clamp_ends(widened, position, devices)
    dz_table = np.arange(layers)[:, None] - np.arange(layers)[None, :] + layers - 1
    kernel_pairs = kernel[:, dz_table]
    cosine, sine = phases(width_cells, width_cells, freq_len, -1.0)
    forward_y = jnp.stack([cosine, sine], axis=1)
    cosine, sine = phases(width_cells, width_cells, freq_len, 1.0)
    weight = jnp.where(jnp.arange(width_cells) == 0, 1.0, 2.0).astype(jnp.float32)[:, None]
    inverse_y = jnp.stack([weight * cosine, -weight * sine], axis=1) / float(track_freq * freq_len)
    damping = material[:, 0].reshape(1, layers, 1, 1)
    nonadiabatic = material[:, 1].reshape(1, layers, 1, 1)
    stiffness = material[:, 2].reshape(1, layers, 1, 1)
    anisotropy = material[:, 3].reshape(1, layers, 1, 1)
    drift_speed = material[:, 4].reshape(1, layers, 1, 1) * region.astype(jnp.float32)[None, None]

    def rate_of(state, widened_in):
        if widened_in is None:
            widened_in = clamp_ends(with_halo(state, ((("gx", "gy"), 2),), 1), position, devices)
        width_pad = jnp.pad(state, ((0, 0), (0, 0), (0, 0), (1, 1)), mode="edge")
        layer_pad = jnp.pad(state, ((0, 0), (1, 1), (0, 0), (0, 0)), mode="edge")
        laplace = widened_in[:, :, 2:] + widened_in[:, :, :-2]
        laplace = laplace + width_pad[:, :, :, 2:] + width_pad[:, :, :, :-2]
        laplace = laplace + layer_pad[:, 2:] + layer_pad[:, :-2] - 6.0 * state
        slope = 0.5 * (widened_in[:, :, 2:] - widened_in[:, :, :-2])
        effective = stiffness * laplace + anisotropy * state[2:3] * fill_up
        effective = effective + demag_field(state, kernel_pairs, forward_y, inverse_y)
        drift_term = drift_speed * slope
        torque_h = cross_product(state, effective)
        damping_h = cross_product(state, torque_h)
        torque_u = cross_product(state, drift_term)
        damping_u = cross_product(state, torque_u)
        change = (
            -torque_h
            - damping * damping_h
            + (1.0 + damping * nonadiabatic) * damping_u
            + (nonadiabatic - damping) * torque_u
        ) / (1.0 + damping * damping)
        return (change, effective)

    section_one, effective_field = rate_of(initial, first_widened)
    section_two, _ = rate_of(initial + 0.5 * time_step * section_one, None)
    section_three, _ = rate_of(initial + 0.5 * time_step * section_two, None)
    section_four, _ = rate_of(initial + time_step * section_three, None)
    magnet_next = initial + time_step / 6.0 * (
        section_one + 2.0 * section_two + 2.0 * section_three + section_four
    )
    return (magnet_next, effective_field)


def split_table(table):
    table = np.asarray(table, np.float64).astype(np.float32)
    high = table.astype(jnp.bfloat16)
    low = (table - high.astype(np.float32)).astype(jnp.bfloat16)
    return np.stack([high, low])


def angle_table(rows, cols, length):
    product = np.outer(np.arange(rows), np.arange(cols)) % length
    return 2.0 * np.pi / length * product


def width_tables(width_cells, devices, scale):
    freq_len = 2 * width_cells - 1
    angles = angle_table(width_cells, width_cells, freq_len)
    shape = (width_cells, devices, 1, width_cells // devices)
    cosine, sine = np.cos(angles).reshape(shape), np.sin(angles).reshape(shape)
    forward = np.concatenate([cosine, -sine], axis=2).reshape(width_cells, 2 * width_cells)
    weight = np.where(np.arange(width_cells) == 0, 1.0, 2.0).reshape(shape[1:]) * scale
    inverse = np.concatenate([weight * cosine, -weight * sine], axis=2)
    return (forward, inverse.reshape(width_cells, 2 * width_cells).T)


def track_tables(track_cells):
    angles = angle_table(track_cells, track_cells, 2 * track_cells)
    cosine, sine = np.cos(angles), np.sin(angles)
    sine[:, 0] = np.where(np.arange(track_cells) % 2 == 0, 1.0, -1.0)
    weight = np.where(np.arange(track_cells) == 0, 1.0, 2.0)
    forward = np.concatenate([cosine, sine], axis=1)
    inverse = np.concatenate([weight * cosine, weight * sine], axis=1)
    return (forward, inverse)


def halves(value):
    high = value.astype(jnp.bfloat16)
    return (high, (value - high.astype(jnp.float32)).astype(jnp.bfloat16))


def dot_halves(left, right, dims=((1,), (0,))):
    def dot(a, b):
        return lax.dot_general(a, b, (dims, ((), ())), preferred_element_type=jnp.float32)

    return dot(left[0], right[0]) + (dot(left[0], right[1]) + dot(left[1], right[0]))


def turn_blocks(blocks, size):
    count = len(blocks)
    group = lax.broadcasted_iota(jnp.int32, blocks[0].shape, 1) // size
    results = []
    for j in range(count):
        result = None
        for i in range(count):
            shift = (i - j) * size % (count * size)
            moved = pltpu.roll(blocks[i], shift, 1) if shift else blocks[i]
            result = moved if result is None else jnp.where(group == i, moved, result)
        results.append(result)
    return results


def send_forward(cells, forward_ref, send_ref, devices):
    slab_rows = send_ref.shape[1]
    size = 2 * forward_ref.shape[1] // devices
    per_tile = lanes // size
    spectrum = dot_halves(halves(cells), (forward_ref[0], forward_ref[1]))
    fields = cells.shape[0] // slab_rows
    for a in range(fields // per_tile):
        for q in range(devices // per_tile):
            blocks = [
                spectrum[(a * per_tile + b) * slab_rows : (a * per_tile + b + 1) * slab_rows, q * lanes : (q + 1) * lanes]
                for b in range(per_tile)
            ]
            for b, block in enumerate(turn_blocks(blocks, size)):
                send_ref[q * per_tile + b, :, a * lanes : (a + 1) * lanes] = block


def take_inverse(received_ref, inverse_ref, rows_ref, fields):
    devices, slab_rows, width = received_ref.shape
    size = inverse_ref.shape[1] // devices
    per_tile = lanes // size
    for a in range(width // lanes):
        for q in range(devices // per_tile):
            blocks = [
                received_ref[q * per_tile + b, :, a * lanes : (a + 1) * lanes] for b in range(per_tile)
            ]
            for b, block in enumerate(turn_blocks(blocks, size)):
                row = (a * per_tile + b) * slab_rows
                rows_ref[row : row + slab_rows, q * lanes : (q + 1) * lanes] = block
    return dot_halves(halves(rows_ref[...]), (inverse_ref[0], inverse_ref[1]))


def first_kernel(devices, magnet_ref, forward_ref, send_ref):
    components, layers, slab_rows, width = magnet_ref.shape
    cells = magnet_ref[...].reshape(components * layers * slab_rows, width)
    send_forward(cells, forward_ref, send_ref, devices)


def window_rows(devices, place_ref, magnet_ref, following_ref, initial_ref, before_ref, after_ref, joined_ref, moved_ref):
    components, layers, slab_rows, width = magnet_ref.shape
    fields = components * layers
    position = place_ref[0]
    offset = place_ref[1]
    limit = devices * slab_rows - offset - position * slab_rows
    joined_ref[:, 0:slab_rows, :] = magnet_ref[...].reshape(fields, slab_rows, width)
    joined_ref[:, slab_rows : 2 * slab_rows, :] = following_ref[...].reshape(fields, slab_rows, width)
    for choice in range(1, slab_rows):

        @pl.when(offset == choice)
        def move():
            for f in range(fields):
                moved_ref[f] = joined_ref[f, choice : choice + slab_rows, :]
                before_ref[f : f + 1, :] = joined_ref[f, choice - 1 : choice, :]
                after_ref[f : f + 1, :] = joined_ref[f, choice + slab_rows : choice + slab_rows + 1, :]

    def filled(rows, cell, field):
        return jnp.where(cell >= limit, jnp.where(field >= fields - layers, 1.0, 0.0), rows)

    rows = moved_ref[...]
    cell = lax.broadcasted_iota(jnp.int32, rows.shape, 1)
    state = filled(rows, cell, lax.broadcasted_iota(jnp.int32, rows.shape, 0))
    initial_ref[...] = state.reshape(components, layers, slab_rows, width)
    edge = lax.broadcasted_iota(jnp.int32, (fields, width), 0)
    before = filled(before_ref[...], jnp.full((fields, width), -1, jnp.int32), edge)
    after = filled(after_ref[...], jnp.full((fields, width), slab_rows, jnp.int32), edge)
    first = jnp.broadcast_to(position, (fields, width)) == 0
    last = jnp.broadcast_to(position, (fields, width)) == devices - 1
    for f in range(fields):
        c, z = divmod(f, layers)
        own = initial_ref[c, z]
        before_ref[f : f + 1, :] = jnp.where(first[0:1], own[0:1], before[f : f + 1])
        after_ref[f : f + 1, :] = jnp.where(last[0:1], own[slab_rows - 1 :], after[f : f + 1])


def track_kernel(stage, fields, *refs):
    refs = list(refs)
    place_ref, fill_ref = [refs.pop(0), refs.pop(0)] if stage == 0 else (None, None)
    received_ref, table_ref, wf_ref, wi_ref, send_ref, spectrum_ref, product_ref = refs[:7]
    devices, slab_rows, width = received_ref.shape
    components = 3
    layers, local_freq = table_ref.shape[1:3]
    track = devices * slab_rows
    flat = received_ref[...].reshape(track, width)
    if stage == 0:
        joined_ref, moved_ref = refs[7:]
        joined_ref[0:track, :] = flat
        joined_ref[track : track + slab_rows, :] = jnp.broadcast_to(fill_ref[place_ref[0]], (slab_rows, width))
        for choice in range(1, slab_rows):

            @pl.when(place_ref[1] == choice)
            def move():
                moved_ref[...] = joined_ref[choice : choice + track, :]

        flat = moved_ref[...]
    else:
        tiles = width // lanes
        for p in range(devices):
            lower = flat[max(p * slab_rows - 1, 0)]
            upper = flat[min(p * slab_rows + slab_rows, track - 1)]
            for a in range(tiles):
                for k, line in enumerate((lower, upper)):
                    value = line[a * lanes : (a + 1) * lanes].reshape(1, lanes)
                    send_ref[p, k * tiles + a : k * tiles + a + 1, width : width + lanes] = value * float(2 * track)
            if 2 * tiles < slab_rows:
                rest = slab_rows - 2 * tiles
                send_ref[p, 2 * tiles : slab_rows, width : width + lanes] = jnp.zeros((rest, lanes), jnp.float32)
    spectrum_ref[...] = dot_halves(halves(flat.T), (wf_ref[0], wf_ref[1]))
    step = 8
    first_lane = lax.broadcasted_iota(jnp.int32, (step, track), 1) == 0
    for start in range(0, local_freq, step):

        def part(j, w, p, half):
            row = ((j * layers + w) * 2 + p) * local_freq + start
            return (slice(row, row + step), slice(half * track, (half + 1) * track))

        tables = {}
        for c in range(6):
            for e in range(layers):
                cosine = table_ref[c, e, start : start + step, 0:track]
                nyquist = table_ref[c, e, start : start + step, track : 2 * track]
                tables[c, e] = (cosine, jnp.where(first_lane, nyquist, cosine) if c in (0, 1, 2, 5) else cosine)
        for i in range(components):
            for z in range(layers):
                sums = [None] * 4

                def add(slot, value, sign):
                    if sums[slot] is None:
                        sums[slot] = value if sign > 0 else -value
                    else:
                        sums[slot] = sums[slot] + value if sign > 0 else sums[slot] - value

                for j in range(components):
                    c = pair_comp[i][j]
                    for w in range(layers):
                        even, odd = tables[c, abs(z - w)]
                        sign = -1 if z < w and c >= 4 else 1
                        ac, as_, bc, bs = [
                            spectrum_ref[part(j, w, p, half)] for p in range(2) for half in range(2)
                        ]
                        if c <= 2:
                            terms = ((even * ac, 1), (odd * as_, 1), (even * bc, 1), (odd * bs, 1))
                        elif c == 3:
                            terms = ((even * bs, 1), (even * bc, -1), (even * as_, -1), (even * ac, 1))
                        elif c == 4:
                            terms = ((even * as_, 1), (even * ac, -1), (even * bs, 1), (even * bc, -1))
                        else:
                            terms = ((even * bc, -1), (odd * bs, -1), (even * ac, 1), (odd * as_, 1))
                        for slot, (value, term_sign) in enumerate(terms):
                            add(slot, value, term_sign * sign)
                for slot in range(4):
                    product_ref[part(i, z, slot // 2, slot % 2)] = sums[slot]
    result = dot_halves((wi_ref[0], wi_ref[1]), halves(product_ref[...]), ((1,), (1,)))
    send_ref[:, :, 0:width] = result.reshape(devices, slab_rows, width)


def step_kernel(stage, devices, place_ref, coef_ref, received_ref, region_ref, inverse_ref, *refs):
    refs = list(refs)
    forward_ref = refs.pop(0) if stage < 3 else None
    if stage == 0:
        magnet_ref, following_ref, field_ref, initial_ref = [refs.pop(0) for _ in range(4)]
        state_ref = initial_ref
    else:
        state_ref, initial_ref, sum_ref = [refs.pop(0) for _ in range(3)]
    next_ref = refs.pop(0)
    if stage < 3:
        total_ref, send_ref = [refs.pop(0) for _ in range(2)]
    rows_ref = refs.pop(0)
    components, layers, slab_rows, width = state_ref.shape
    if stage == 0:
        before_ref, after_ref = refs[:2]
        window_rows(devices, place_ref, magnet_ref, following_ref, initial_ref, *refs)
    demag = take_inverse(received_ref, inverse_ref, rows_ref, components * layers)
    tiles = 2 * width * components * layers // (devices * lanes)
    per_tile = components * layers // tiles
    shape = (slab_rows, width)
    row = lax.broadcasted_iota(jnp.int32, shape, 0)
    col = lax.broadcasted_iota(jnp.int32, shape, 1)
    flow = region_ref[...].astype(jnp.float32)
    for z in range(layers):
        stiffness, anisotropy, drift = (coef_ref[z, 4], coef_ref[z, 5], coef_ref[z, 6])
        m, h, g = ([], [], [])
        for c in range(components):
            f = c * layers + z
            cells = state_ref[c, z]
            if stage == 0:
                head, tail = (before_ref[f : f + 1, :], after_ref[f : f + 1, :])
            else:
                line = (components * layers + f % per_tile) * slab_rows + f // per_tile
                head, tail = (demag[line : line + 1], demag[line + tiles : line + tiles + 1])
            lower = jnp.where(row == 0, head, pltpu.roll(cells, 1, 0))
            upper = jnp.where(row == slab_rows - 1, tail, pltpu.roll(cells, slab_rows - 1, 0))
            left = jnp.where(col == 0, cells, pltpu.roll(cells, 1, 1))
            right = jnp.where(col == width - 1, cells, pltpu.roll(cells, width - 1, 1))
            laplace = (upper + lower) + (left + right)
            laplace = laplace + state_ref[c, max(z - 1, 0)] + state_ref[c, min(z + 1, layers - 1)] - 6.0 * cells
            effective = stiffness * laplace + demag[f * slab_rows : (f + 1) * slab_rows, :]
            if c == 2:
                effective = effective + anisotropy * cells
            if stage == 0:
                field_ref[c, z] = effective
            m.append(cells)
            h.append(effective)
            g.append((0.5 * drift) * flow * (upper - lower))
        inner = [coef_ref[z, 1] * h[c] + coef_ref[z, 2] * g[c] for c in range(3)]
        outer = [coef_ref[z, 0] * h[c] + coef_ref[z, 3] * g[c] for c in range(3)]
        turned = [m[(c + 1) % 3] * inner[(c + 2) % 3] - m[(c + 2) % 3] * inner[(c + 1) % 3] for c in range(3)]
        whole = [outer[c] + turned[c] for c in range(3)]
        for c in range(components):
            rate = m[(c + 1) % 3] * whole[(c + 2) % 3] - m[(c + 2) % 3] * whole[(c + 1) % 3]
            start = initial_ref[c, z]
            if stage == 3:
                next_ref[c, z] = start + (time_step / 6.0) * (sum_ref[c, z] + rate)
            else:
                factor = time_step if stage == 2 else 0.5 * time_step
                value = start + factor * rate
                next_ref[c, z] = value
                total_ref[c, z] = rate if stage == 0 else sum_ref[c, z] + 2.0 * rate
    if stage < 3:
        cells = next_ref[...].reshape(components * layers * slab_rows, width)
        send_forward(cells, forward_ref, send_ref, devices)


def call(body, name, outs, in_smem, args, scratch):
    in_specs = [
        pl.BlockSpec(memory_space=pltpu.SMEM if i < in_smem else pltpu.VMEM) for i in range(len(args))
    ]
    return pl.pallas_call(
        body,
        name=name,
        out_shape=[jax.ShapeDtypeStruct(s, jnp.float32) for s in outs],
        in_specs=in_specs,
        out_specs=[pl.BlockSpec(memory_space=pltpu.VMEM) for _ in outs],
        scratch_shapes=[pltpu.VMEM(s, jnp.float32) for s in scratch],
        compiler_params=pltpu.CompilerParams(vmem_limit_bytes=24 * 1024 * 1024),
    )(*args)


def exchange(blocks):
    return lax.all_to_all(blocks, ("gx", "gy"), split_axis=0, concat_axis=0, tiled=True)


def local_tiled(magnet, window_shift, region, material, kernel):
    components, layers, slab_rows, width = magnet.shape
    devices = lax.axis_size(("gx", "gy"))
    position = lax.axis_index(("gx", "gy"))
    track = slab_rows * devices
    fields = components * layers
    scale = 1.0 / (2 * track * (2 * width - 1))
    forward, inverse = [split_table(t) for t in width_tables(width, devices, scale)]
    track_forward, track_inverse = [split_table(t) for t in track_tables(track)]
    row_width = 2 * fields * (width // devices)
    block_shape = (devices, slab_rows, row_width)
    following = passed_along(magnet, ("gx", "gy"), -1)
    place = jnp.stack([position.astype(jnp.int32), window_shift[0]])
    a, b = (material[:, 0], material[:, 1])
    below = 1.0 / (1.0 + a * a)
    zero = jnp.zeros_like(a)
    coef = jnp.stack(
        [-below, -a * below, (1.0 + a * b) * below, (b - a) * below, material[:, 2], material[:, 3], material[:, 4], zero],
        axis=1,
    )
    table = kernel[:, layers - 1 :]
    ones = np.zeros((components, layers, 2, width // devices, devices))
    sums = width_tables(width, devices, scale)[0].sum(axis=0).reshape(devices, 2, width // devices)
    ones[2] = np.transpose(sums, (1, 2, 0))
    fill = np.transpose(ones.reshape(row_width, devices)).reshape(devices, 1, row_width).astype(np.float32)
    (send,) = call(
        functools.partial(first_kernel, devices), "first", [block_shape], 0, [magnet, forward], []
    )
    tiles = row_width // lanes
    per_tile = fields // tiles
    wide_shape = (devices, slab_rows, row_width + lanes)
    state = None
    for stage in range(4):
        received = exchange(send)
        args = [received, table, track_forward, track_inverse]
        scratch = [(row_width, 2 * track), (row_width, 2 * track)]
        if stage == 0:
            args = [place, fill] + args
            scratch += [(track + slab_rows, row_width), (track, row_width)]
        (back,) = call(
            functools.partial(track_kernel, stage, fields),
            "track",
            [wide_shape if stage > 0 else block_shape],
            1 if stage == 0 else 0,
            args,
            scratch,
        )
        returned = exchange(back)
        args = [place, coef, returned, region, inverse]
        outs = [magnet.shape]
        scratch = [(fields * slab_rows + (per_tile * slab_rows if stage > 0 else 0), 2 * width)]
        if stage < 3:
            args += [forward]
            outs += [magnet.shape, block_shape]
        if stage > 0:
            args += [state, initial, total]
        else:
            args += [magnet, following]
            outs = [magnet.shape, magnet.shape] + outs
            scratch += [(fields, width), (fields, width), (fields, 2 * slab_rows, width), (fields, slab_rows, width)]
        results = list(call(functools.partial(step_kernel, stage, devices), "step", outs, 2, args, scratch))
        if stage == 0:
            effective_field = results.pop(0)
            initial = results.pop(0)
        state = results.pop(0)
        if stage < 3:
            total, send = results
    return (state, effective_field)


def fits_tiles(mesh_devices, width):
    size = 2 * (width // mesh_devices)
    return size % 16 == 0 and lanes % size == 0 and mesh_devices % (lanes // size) == 0


def local_any(magnet, window_shift, region, material, kernel):
    components, layers, slab_rows, width = magnet.shape
    devices = lax.axis_size(("gx", "gy"))
    track = slab_rows * devices
    per_tile = lanes * devices // (2 * width)
    tiled = fits_tiles(devices, width) and slab_rows % 8 == 0 and track % lanes == 0 and width % lanes == 0
    tiled = tiled and components * layers % max(per_tile, 1) == 0
    tiled = tiled and 2 * components * layers <= slab_rows * max(per_tile, 1)
    return (local_tiled if tiled else local)(magnet, window_shift, region, material, kernel)


def solution(mesh):
    in_specs = (
        P(None, None, ("run", "gx", "gy"), None),
        P("run"),
        P(("run", "gx", "gy"), None),
        P(),
        P(None, None, ("gx", "gy"), None),
    )
    out_specs = (P(None, None, ("run", "gx", "gy"), None), P(None, None, ("run", "gx", "gy"), None))
    return jax.shard_map(local_any, mesh=mesh, in_specs=in_specs, out_specs=out_specs, check_vma=False)
```

```python
import functools
import math

import jax
import jax.numpy as jnp
import numpy as np
from jax import lax
from jax.experimental import pallas as pl
from jax.experimental.pallas import tpu as pltpu
from jax.sharding import PartitionSpec as P

time_step = 0.1
pair_comp = ((0, 3, 4), (3, 1, 5), (4, 5, 2))
highest = lax.Precision.HIGHEST
lanes = 128


def passed_along(value, axis, steps):
    count = lax.axis_size(axis)
    leading, last = (max(0, -steps), min(count, count - steps))
    return lax.ppermute(value, axis, [(source, source + steps) for source in range(leading, last)])


def with_halo(cells, sides, width):
    for axis, dim in sides:
        count = lax.axis_size(axis)
        ends = count - 1
        head = lax.slice_in_dim(cells, 0, width, axis=dim)
        tail = lax.slice_in_dim(cells, cells.shape[dim] - width, cells.shape[dim], axis=dim)
        cells = jnp.concatenate(
            [
                lax.ppermute(tail, axis, [(i, (i + 1) % count) for i in range(ends)]),
                cells,
                lax.ppermute(head, axis, [((i + 1) % count, i) for i in range(ends)]),
            ],
            axis=dim,
        )
    return cells


def cross_product(left, right):
    return jnp.stack(
        [
            left[1] * right[2] - left[2] * right[1],
            left[2] * right[0] - left[0] * right[2],
            left[0] * right[1] - left[1] * right[0],
        ]
    )


def phases(count_rows, count_cols, length, direction):
    product = (
        jnp.arange(count_rows, dtype=jnp.int32)[:, None]
        * jnp.arange(count_cols, dtype=jnp.int32)[None, :]
        % length
    )
    angles = direction * 2.0 * math.pi / length * product.astype(jnp.float32)
    return (jnp.cos(angles), jnp.sin(angles))


def complex_table(cosine, sine):
    top_rows = jnp.stack([cosine, sine], axis=1)
    bottom_rows = jnp.stack([-sine, cosine], axis=1)
    return jnp.stack([top_rows, bottom_rows], axis=0)


def twist(first_pass, cosine, sine):
    real_part = first_pass[:, 0]
    imag_part = first_pass[:, 1]
    return jnp.stack(
        [real_part * cosine - imag_part * sine, real_part * sine + imag_part * cosine], axis=1
    )


def forward_track(values):
    batch, pair, track_cells = values.shape
    track_freq = 2 * track_cells
    outer_len = track_freq // 64
    outer_used = track_cells // 64
    blocked = values.reshape(batch, 2, outer_used, 64)
    cosine, sine = phases(outer_used, outer_len, outer_len, -1.0)
    first_pass = jnp.einsum(
        "bpxa,pxqk->bqka", blocked, complex_table(cosine, sine), precision=highest
    )
    twist_cos, twist_sin = phases(outer_len, 64, track_freq, -1.0)
    twisted = twist(first_pass, twist_cos, twist_sin)
    cosine, sine = phases(64, 64, 64, -1.0)
    result = jnp.einsum("bpka,paqj->bqjk", twisted, complex_table(cosine, sine), precision=highest)
    return result.reshape(batch, 2, track_freq)


def inverse_track(values):
    batch, pair, track_freq = values.shape
    track_cells = track_freq // 2
    outer_len = track_freq // 64
    outer_used = track_cells // 64
    blocked = values.reshape(batch, 2, 64, outer_len)
    cosine, sine = phases(64, 64, 64, 1.0)
    first_pass = jnp.einsum(
        "bpjk,pjqa->bqka", blocked, complex_table(cosine, sine), precision=highest
    )
    twist_cos, twist_sin = phases(outer_len, 64, track_freq, 1.0)
    twisted = twist(first_pass, twist_cos, twist_sin)
    cosine, sine = phases(outer_len, outer_used, outer_len, 1.0)
    result = jnp.einsum("bpka,pkqx->bqxa", twisted, complex_table(cosine, sine), precision=highest)
    return result.reshape(batch, 2, track_cells)


def apply_kernel(spectrum, kernel_pairs):
    fields = []
    for i in range(3):
        summed = None
        for j in range(3):
            index_c = pair_comp[i][j]
            table = kernel_pairs[index_c][:, :, :, None, :]
            contrib = jnp.sum(table * spectrum[j][None], axis=1)
            if index_c >= 4:
                contrib = jnp.stack([-contrib[:, :, 1], contrib[:, :, 0]], axis=2)
            summed = contrib if summed is None else summed + contrib
        fields.append(summed)
    return jnp.stack(fields)


def clamp_ends(widened, position, devices):
    head_row = jnp.where(position == 0, widened[:, :, 1:2], widened[:, :, 0:1])
    tail_row = jnp.where(position == devices - 1, widened[:, :, -2:-1], widened[:, :, -1:])
    return jnp.concatenate([head_row, widened[:, :, 1:-1], tail_row], axis=2)


def demag_field(state, kernel_pairs, forward_y, inverse_y):
    components, layers, slab_rows, width_cells = state.shape
    devices = lax.axis_size(("gx", "gy"))
    local_freq = width_cells // devices
    track_cells = slab_rows * devices
    track_freq = 2 * track_cells
    spectrum = jnp.einsum("czxy,ypk->czkpx", state, forward_y, precision=highest)
    blocks = spectrum.reshape(components, layers, devices, local_freq, 2, 1, slab_rows)
    arrived = lax.all_to_all(blocks, ("gx", "gy"), split_axis=2, concat_axis=5, tiled=True)
    flat_rows = arrived.reshape(components * layers * local_freq, 2, track_cells)
    spectrum_x = forward_track(flat_rows).reshape(components, layers, local_freq, 2, track_freq)
    product_hat = apply_kernel(spectrum_x, kernel_pairs)
    returned_x = inverse_track(product_hat.reshape(components * layers * local_freq, 2, track_freq))
    pieces = returned_x.reshape(components, layers, 1, local_freq, 2, devices, slab_rows)
    landed = lax.all_to_all(pieces, ("gx", "gy"), split_axis=5, concat_axis=2, tiled=True)
    gathered_y = landed.reshape(components, layers, width_cells, 2, slab_rows)
    return jnp.einsum("czkpx,kpy->czxy", gathered_y, inverse_y, precision=highest)


def local(magnet, window_shift, region, material, kernel):
    components, layers, slab_rows, width_cells = magnet.shape
    devices = lax.axis_size(("gx", "gy"))
    position = lax.axis_index(("gx", "gy"))
    track_cells = slab_rows * devices
    track_freq = 2 * track_cells
    freq_len = 2 * width_cells - 1
    offset = window_shift[0]
    fill_up = (jnp.arange(3) == 2).astype(jnp.float32).reshape(3, 1, 1, 1)
    following = passed_along(magnet, ("gx", "gy"), -1)
    joined = jnp.concatenate([magnet, following], axis=2)
    widened = lax.dynamic_slice_in_dim(joined, offset - 1, slab_rows + 2, 2)
    global_cell = position * slab_rows - 1 + jnp.arange(slab_rows + 2, dtype=jnp.int32)
    widened = jnp.where(
        (global_cell >= track_cells - offset)[None, None, :, None], fill_up, widened
    )
    initial = widened[:, :, 1:-1]
    first_widened = clamp_ends(widened, position, devices)
    dz_table = np.arange(layers)[:, None] - np.arange(layers)[None, :] + layers - 1
    kernel_pairs = kernel[:, dz_table]
    cosine, sine = phases(width_cells, width_cells, freq_len, -1.0)
    forward_y = jnp.stack([cosine, sine], axis=1)
    cosine, sine = phases(width_cells, width_cells, freq_len, 1.0)
    weight = jnp.where(jnp.arange(width_cells) == 0, 1.0, 2.0).astype(jnp.float32)[:, None]
    inverse_y = jnp.stack([weight * cosine, -weight * sine], axis=1) / float(track_freq * freq_len)
    damping = material[:, 0].reshape(1, layers, 1, 1)
    nonadiabatic = material[:, 1].reshape(1, layers, 1, 1)
    stiffness = material[:, 2].reshape(1, layers, 1, 1)
    anisotropy = material[:, 3].reshape(1, layers, 1, 1)
    drift_speed = material[:, 4].reshape(1, layers, 1, 1) * region.astype(jnp.float32)[None, None]

    def rate_of(state, widened_in):
        if widened_in is None:
            widened_in = clamp_ends(with_halo(state, ((("gx", "gy"), 2),), 1), position, devices)
        width_pad = jnp.pad(state, ((0, 0), (0, 0), (0, 0), (1, 1)), mode="edge")
        layer_pad = jnp.pad(state, ((0, 0), (1, 1), (0, 0), (0, 0)), mode="edge")
        laplace = widened_in[:, :, 2:] + widened_in[:, :, :-2]
        laplace = laplace + width_pad[:, :, :, 2:] + width_pad[:, :, :, :-2]
        laplace = laplace + layer_pad[:, 2:] + layer_pad[:, :-2] - 6.0 * state
        slope = 0.5 * (widened_in[:, :, 2:] - widened_in[:, :, :-2])
        effective = stiffness * laplace + anisotropy * state[2:3] * fill_up
        effective = effective + demag_field(state, kernel_pairs, forward_y, inverse_y)
        drift_term = drift_speed * slope
        torque_h = cross_product(state, effective)
        damping_h = cross_product(state, torque_h)
        torque_u = cross_product(state, drift_term)
        damping_u = cross_product(state, torque_u)
        change = (
            -torque_h
            - damping * damping_h
            + (1.0 + damping * nonadiabatic) * damping_u
            + (nonadiabatic - damping) * torque_u
        ) / (1.0 + damping * damping)
        return (change, effective)

    section_one, effective_field = rate_of(initial, first_widened)
    section_two, _ = rate_of(initial + 0.5 * time_step * section_one, None)
    section_three, _ = rate_of(initial + 0.5 * time_step * section_two, None)
    section_four, _ = rate_of(initial + time_step * section_three, None)
    magnet_next = initial + time_step / 6.0 * (
        section_one + 2.0 * section_two + 2.0 * section_three + section_four
    )
    return (magnet_next, effective_field)


def split_table(table):
    table = np.asarray(table, np.float64).astype(np.float32)
    high = table.astype(jnp.bfloat16)
    low = (table - high.astype(np.float32)).astype(jnp.bfloat16)
    return np.stack([high, low])


def angle_table(rows, cols, length):
    product = np.outer(np.arange(rows), np.arange(cols)) % length
    return 2.0 * np.pi / length * product


def width_tables(width_cells, devices, scale):
    freq_len = 2 * width_cells - 1
    angles = angle_table(width_cells, width_cells, freq_len)
    shape = (width_cells, devices, 1, width_cells // devices)
    cosine, sine = np.cos(angles).reshape(shape), np.sin(angles).reshape(shape)
    forward = np.concatenate([cosine, -sine], axis=2).reshape(width_cells, 2 * width_cells)
    weight = np.where(np.arange(width_cells) == 0, 1.0, 2.0).reshape(shape[1:]) * scale
    inverse = np.concatenate([weight * cosine, -weight * sine], axis=2)
    return (forward, inverse.reshape(width_cells, 2 * width_cells).T)


def track_tables(track_cells):
    angles = angle_table(track_cells, track_cells, 2 * track_cells)
    cosine, sine = np.cos(angles), np.sin(angles)
    sine[:, 0] = np.where(np.arange(track_cells) % 2 == 0, 1.0, -1.0)
    weight = np.where(np.arange(track_cells) == 0, 1.0, 2.0)
    forward = np.concatenate([cosine, sine], axis=1)
    inverse = np.concatenate([weight * cosine, weight * sine], axis=1)
    return (forward, inverse)


def halves(value):
    high = value.astype(jnp.bfloat16)
    return (high, (value - high.astype(jnp.float32)).astype(jnp.bfloat16))


def dot_halves(left, right, dims=((1,), (0,))):
    def dot(a, b):
        return lax.dot_general(a, b, (dims, ((), ())), preferred_element_type=jnp.float32)

    rows = left[0].shape[0]
    both = dot(jnp.concatenate([left[0], left[1]], axis=0), right[0])
    return both[:rows] + (both[rows:] + dot(left[0], right[1]))


def turn_blocks(blocks, size):
    count = len(blocks)
    group = lax.broadcasted_iota(jnp.int32, blocks[0].shape, 1) // size
    results = []
    for j in range(count):
        result = None
        for i in range(count):
            shift = (i - j) * size % (count * size)
            moved = pltpu.roll(blocks[i], shift, 1) if shift else blocks[i]
            result = moved if result is None else jnp.where(group == i, moved, result)
        results.append(result)
    return results


def send_forward(cells, forward_ref, send_ref, devices):
    slab_rows = send_ref.shape[1]
    size = 2 * forward_ref.shape[1] // devices
    per_tile = lanes // size
    spectrum = dot_halves(halves(cells), (forward_ref[0], forward_ref[1]))
    fields = cells.shape[0] // slab_rows
    for a in range(fields // per_tile):
        for q in range(devices // per_tile):
            blocks = [
                spectrum[(a * per_tile + b) * slab_rows : (a * per_tile + b + 1) * slab_rows, q * lanes : (q + 1) * lanes]
                for b in range(per_tile)
            ]
            for b, block in enumerate(turn_blocks(blocks, size)):
                send_ref[q * per_tile + b, :, a * lanes : (a + 1) * lanes] = block


def take_inverse(received_ref, inverse_ref, rows_ref, fields):
    devices, slab_rows, width = received_ref.shape
    size = inverse_ref.shape[1] // devices
    per_tile = lanes // size
    for a in range(width // lanes):
        for q in range(devices // per_tile):
            blocks = [
                received_ref[q * per_tile + b, :, a * lanes : (a + 1) * lanes] for b in range(per_tile)
            ]
            for b, block in enumerate(turn_blocks(blocks, size)):
                row = (a * per_tile + b) * slab_rows
                rows_ref[row : row + slab_rows, q * lanes : (q + 1) * lanes] = block
    return dot_halves(halves(rows_ref[...]), (inverse_ref[0], inverse_ref[1]))


def first_kernel(devices, magnet_hbm, forward_hbm, send_ref, magnet_ref, forward_ref, sems):
    copies = [
        pltpu.make_async_copy(magnet_hbm, magnet_ref, sems.at[0]),
        pltpu.make_async_copy(forward_hbm, forward_ref, sems.at[1]),
    ]
    for copy in copies:
        copy.start()
    for copy in copies:
        copy.wait()
    components, layers, slab_rows, width = magnet_ref.shape
    cells = magnet_ref[...].reshape(components * layers * slab_rows, width)
    send_forward(cells, forward_ref, send_ref, devices)


def window_rows(devices, place_ref, magnet_ref, following_ref, initial_ref, before_ref, after_ref, joined_ref, moved_ref):
    components, layers, slab_rows, width = magnet_ref.shape
    fields = components * layers
    position = place_ref[0]
    offset = place_ref[1]
    limit = devices * slab_rows - offset - position * slab_rows
    joined_ref[:, 0:slab_rows, :] = magnet_ref[...].reshape(fields, slab_rows, width)
    joined_ref[:, slab_rows : 2 * slab_rows, :] = following_ref[...].reshape(fields, slab_rows, width)
    for choice in range(1, slab_rows):

        @pl.when(offset == choice)
        def move():
            for f in range(fields):
                moved_ref[f] = joined_ref[f, choice : choice + slab_rows, :]
                before_ref[f : f + 1, :] = joined_ref[f, choice - 1 : choice, :]
                after_ref[f : f + 1, :] = joined_ref[f, choice + slab_rows : choice + slab_rows + 1, :]

    def filled(rows, cell, field):
        return jnp.where(cell >= limit, jnp.where(field >= fields - layers, 1.0, 0.0), rows)

    rows = moved_ref[...]
    cell = lax.broadcasted_iota(jnp.int32, rows.shape, 1)
    state = filled(rows, cell, lax.broadcasted_iota(jnp.int32, rows.shape, 0))
    initial_ref[...] = state.reshape(components, layers, slab_rows, width)
    edge = lax.broadcasted_iota(jnp.int32, (fields, width), 0)
    before = filled(before_ref[...], jnp.full((fields, width), -1, jnp.int32), edge)
    after = filled(after_ref[...], jnp.full((fields, width), slab_rows, jnp.int32), edge)
    first = jnp.broadcast_to(position, (fields, width)) == 0
    last = jnp.broadcast_to(position, (fields, width)) == devices - 1
    for f in range(fields):
        c, z = divmod(f, layers)
        own = initial_ref[c, z]
        before_ref[f : f + 1, :] = jnp.where(first[0:1], own[0:1], before[f : f + 1])
        after_ref[f : f + 1, :] = jnp.where(last[0:1], own[slab_rows - 1 :], after[f : f + 1])


def track_kernel(stage, fields, *refs):
    refs = list(refs)
    place_ref, fill_ref = [refs.pop(0), refs.pop(0)] if stage == 0 else (None, None)
    received_ref, table_ref, wf_ref, wi_ref, send_ref, spectrum_ref, product_ref = refs[:7]
    devices, slab_rows, width = received_ref.shape
    components = 3
    layers, local_freq = table_ref.shape[1:3]
    track = devices * slab_rows
    flat = received_ref[...].reshape(track, width)
    if stage == 0:
        joined_ref, moved_ref = refs[7:]
        joined_ref[0:track, :] = flat
        joined_ref[track : track + slab_rows, :] = jnp.broadcast_to(fill_ref[place_ref[0]], (slab_rows, width))
        for choice in range(1, slab_rows):

            @pl.when(place_ref[1] == choice)
            def move():
                moved_ref[...] = joined_ref[choice : choice + track, :]

        flat = moved_ref[...]
    else:
        tiles = width // lanes
        for p in range(devices):
            lower = flat[max(p * slab_rows - 1, 0)]
            upper = flat[min(p * slab_rows + slab_rows, track - 1)]
            for a in range(tiles):
                for k, line in enumerate((lower, upper)):
                    value = line[a * lanes : (a + 1) * lanes].reshape(1, lanes)
                    send_ref[p, k * tiles + a : k * tiles + a + 1, width : width + lanes] = value * float(2 * track)
            if 2 * tiles < slab_rows:
                rest = slab_rows - 2 * tiles
                send_ref[p, 2 * tiles : slab_rows, width : width + lanes] = jnp.zeros((rest, lanes), jnp.float32)
    spectrum_ref[...] = dot_halves(halves(flat.T), (wf_ref[0], wf_ref[1]))
    step = 8
    first_lane = lax.broadcasted_iota(jnp.int32, (step, track), 1) == 0
    for start in range(0, local_freq, step):

        def part(j, w, p, half):
            row = ((j * layers + w) * 2 + p) * local_freq + start
            return (slice(row, row + step), slice(half * track, (half + 1) * track))

        tables = {}
        for c in range(6):
            for e in range(layers):
                cosine = table_ref[c, e, start : start + step, 0:track]
                nyquist = table_ref[c, e, start : start + step, track : 2 * track]
                tables[c, e] = (cosine, jnp.where(first_lane, nyquist, cosine) if c in (0, 1, 2, 5) else cosine)
        for i in range(components):
            for z in range(layers):
                sums = [None] * 4

                def add(slot, value, sign):
                    if sums[slot] is None:
                        sums[slot] = value if sign > 0 else -value
                    else:
                        sums[slot] = sums[slot] + value if sign > 0 else sums[slot] - value

                for j in range(components):
                    c = pair_comp[i][j]
                    for w in range(layers):
                        even, odd = tables[c, abs(z - w)]
                        sign = -1 if z < w and c >= 4 else 1
                        ac, as_, bc, bs = [
                            spectrum_ref[part(j, w, p, half)] for p in range(2) for half in range(2)
                        ]
                        if c <= 2:
                            terms = ((even * ac, 1), (odd * as_, 1), (even * bc, 1), (odd * bs, 1))
                        elif c == 3:
                            terms = ((even * bs, 1), (even * bc, -1), (even * as_, -1), (even * ac, 1))
                        elif c == 4:
                            terms = ((even * as_, 1), (even * ac, -1), (even * bs, 1), (even * bc, -1))
                        else:
                            terms = ((even * bc, -1), (odd * bs, -1), (even * ac, 1), (odd * as_, 1))
                        for slot, (value, term_sign) in enumerate(terms):
                            add(slot, value, term_sign * sign)
                for slot in range(4):
                    product_ref[part(i, z, slot // 2, slot % 2)] = sums[slot]
    result = dot_halves((wi_ref[0], wi_ref[1]), halves(product_ref[...]), ((1,), (1,)))
    send_ref[:, :, 0:width] = result.reshape(devices, slab_rows, width)


def step_kernel(stage, devices, place_ref, coef_ref, received_ref, region_ref, inverse_ref, *refs):
    refs = list(refs)
    forward_ref = refs.pop(0) if stage < 3 else None
    if stage == 0:
        magnet_ref, following_ref, field_ref, initial_ref = [refs.pop(0) for _ in range(4)]
        state_ref = initial_ref
    else:
        state_ref, initial_ref, sum_ref = [refs.pop(0) for _ in range(3)]
    next_ref = refs.pop(0)
    if stage < 3:
        total_ref, send_ref = [refs.pop(0) for _ in range(2)]
    rows_ref = refs.pop(0)
    components, layers, slab_rows, width = state_ref.shape
    if stage == 0:
        before_ref, after_ref = refs[:2]
        window_rows(devices, place_ref, magnet_ref, following_ref, initial_ref, *refs)
    demag = take_inverse(received_ref, inverse_ref, rows_ref, components * layers)
    tiles = 2 * width * components * layers // (devices * lanes)
    per_tile = components * layers // tiles
    shape = (slab_rows, width)
    row = lax.broadcasted_iota(jnp.int32, shape, 0)
    col = lax.broadcasted_iota(jnp.int32, shape, 1)
    flow = region_ref[...].astype(jnp.float32)
    for z in range(layers):
        stiffness, anisotropy, drift = (coef_ref[z, 4], coef_ref[z, 5], coef_ref[z, 6])
        m, h, g = ([], [], [])
        for c in range(components):
            f = c * layers + z
            cells = state_ref[c, z]
            if stage == 0:
                head, tail = (before_ref[f : f + 1, :], after_ref[f : f + 1, :])
            else:
                line = (components * layers + f % per_tile) * slab_rows + f // per_tile
                head, tail = (demag[line : line + 1], demag[line + tiles : line + tiles + 1])
            lower = jnp.where(row == 0, head, pltpu.roll(cells, 1, 0))
            upper = jnp.where(row == slab_rows - 1, tail, pltpu.roll(cells, slab_rows - 1, 0))
            left = jnp.where(col == 0, cells, pltpu.roll(cells, 1, 1))
            right = jnp.where(col == width - 1, cells, pltpu.roll(cells, width - 1, 1))
            laplace = (upper + lower) + (left + right)
            laplace = laplace + state_ref[c, max(z - 1, 0)] + state_ref[c, min(z + 1, layers - 1)] - 6.0 * cells
            effective = stiffness * laplace + demag[f * slab_rows : (f + 1) * slab_rows, :]
            if c == 2:
                effective = effective + anisotropy * cells
            if stage == 0:
                field_ref[c, z] = effective
            m.append(cells)
            h.append(effective)
            g.append((0.5 * drift) * flow * (upper - lower))
        inner = [coef_ref[z, 1] * h[c] + coef_ref[z, 2] * g[c] for c in range(3)]
        outer = [coef_ref[z, 0] * h[c] + coef_ref[z, 3] * g[c] for c in range(3)]
        turned = [m[(c + 1) % 3] * inner[(c + 2) % 3] - m[(c + 2) % 3] * inner[(c + 1) % 3] for c in range(3)]
        whole = [outer[c] + turned[c] for c in range(3)]
        for c in range(components):
            rate = m[(c + 1) % 3] * whole[(c + 2) % 3] - m[(c + 2) % 3] * whole[(c + 1) % 3]
            start = initial_ref[c, z]
            if stage == 3:
                next_ref[c, z] = start + (time_step / 6.0) * (sum_ref[c, z] + rate)
            else:
                factor = time_step if stage == 2 else 0.5 * time_step
                value = start + factor * rate
                next_ref[c, z] = value
                total_ref[c, z] = rate if stage == 0 else sum_ref[c, z] + 2.0 * rate
    if stage < 3:
        cells = next_ref[...].reshape(components * layers * slab_rows, width)
        send_forward(cells, forward_ref, send_ref, devices)


def call(body, name, outs, in_smem, args, scratch):
    in_specs = [
        pl.BlockSpec(memory_space=pltpu.SMEM if i < in_smem else pltpu.VMEM) for i in range(len(args))
    ]
    return pl.pallas_call(
        body,
        name=name,
        out_shape=[jax.ShapeDtypeStruct(s, jnp.float32) for s in outs],
        in_specs=in_specs,
        out_specs=[pl.BlockSpec(memory_space=pltpu.VMEM) for _ in outs],
        scratch_shapes=[pltpu.VMEM(s, jnp.float32) for s in scratch],
        compiler_params=pltpu.CompilerParams(vmem_limit_bytes=24 * 1024 * 1024),
    )(*args)


def exchange(blocks):
    return lax.all_to_all(blocks, ("gx", "gy"), split_axis=0, concat_axis=0, tiled=True)


def local_tiled(magnet, window_shift, region, material, kernel):
    components, layers, slab_rows, width = magnet.shape
    devices = lax.axis_size(("gx", "gy"))
    position = lax.axis_index(("gx", "gy"))
    track = slab_rows * devices
    fields = components * layers
    scale = 1.0 / (2 * track * (2 * width - 1))
    forward, inverse = [split_table(t) for t in width_tables(width, devices, scale)]
    track_forward, track_inverse = [split_table(t) for t in track_tables(track)]
    row_width = 2 * fields * (width // devices)
    block_shape = (devices, slab_rows, row_width)
    following = passed_along(magnet, ("gx", "gy"), -1)
    place = jnp.stack([position.astype(jnp.int32), window_shift[0]])
    a, b = (material[:, 0], material[:, 1])
    below = 1.0 / (1.0 + a * a)
    zero = jnp.zeros_like(a)
    coef = jnp.stack(
        [-below, -a * below, (1.0 + a * b) * below, (b - a) * below, material[:, 2], material[:, 3], material[:, 4], zero],
        axis=1,
    )
    table = kernel[:, layers - 1 :]
    ones = np.zeros((components, layers, 2, width // devices, devices))
    sums = width_tables(width, devices, scale)[0].sum(axis=0).reshape(devices, 2, width // devices)
    ones[2] = np.transpose(sums, (1, 2, 0))
    fill = np.transpose(ones.reshape(row_width, devices)).reshape(devices, 1, row_width).astype(np.float32)
    send = pl.pallas_call(
        functools.partial(first_kernel, devices),
        name="first",
        out_shape=jax.ShapeDtypeStruct(block_shape, jnp.float32),
        in_specs=[pl.BlockSpec(memory_space=pltpu.HBM)] * 2,
        out_specs=pl.BlockSpec(memory_space=pltpu.VMEM),
        scratch_shapes=[
            pltpu.VMEM(magnet.shape, jnp.float32),
            pltpu.VMEM(forward.shape, jnp.bfloat16),
            pltpu.SemaphoreType.DMA((2,)),
        ],
        compiler_params=pltpu.CompilerParams(vmem_limit_bytes=24 * 1024 * 1024),
    )(magnet, forward)
    tiles = row_width // lanes
    per_tile = fields // tiles
    wide_shape = (devices, slab_rows, row_width + lanes)
    state = None
    for stage in range(4):
        received = exchange(send)
        args = [received, table, track_forward, track_inverse]
        scratch = [(row_width, 2 * track), (row_width, 2 * track)]
        if stage == 0:
            args = [place, fill] + args
            scratch += [(track + slab_rows, row_width), (track, row_width)]
        (back,) = call(
            functools.partial(track_kernel, stage, fields),
            "track",
            [wide_shape if stage > 0 else block_shape],
            1 if stage == 0 else 0,
            args,
            scratch,
        )
        returned = exchange(back)
        args = [place, coef, returned, region, inverse]
        outs = [magnet.shape]
        scratch = [(fields * slab_rows + (per_tile * slab_rows if stage > 0 else 0), 2 * width)]
        if stage < 3:
            args += [forward]
            outs += [magnet.shape, block_shape]
        if stage > 0:
            args += [state, initial, total]
        else:
            args += [magnet, following]
            outs = [magnet.shape, magnet.shape] + outs
            scratch += [(fields, width), (fields, width), (fields, 2 * slab_rows, width), (fields, slab_rows, width)]
        results = list(call(functools.partial(step_kernel, stage, devices), "step", outs, 2, args, scratch))
        if stage == 0:
            effective_field = results.pop(0)
            initial = results.pop(0)
        state = results.pop(0)
        if stage < 3:
            total, send = results
    return (state, effective_field)


def fits_tiles(mesh_devices, width):
    size = 2 * (width // mesh_devices)
    return size % 16 == 0 and lanes % size == 0 and mesh_devices % (lanes // size) == 0


def local_any(magnet, window_shift, region, material, kernel):
    components, layers, slab_rows, width = magnet.shape
    devices = lax.axis_size(("gx", "gy"))
    track = slab_rows * devices
    per_tile = lanes * devices // (2 * width)
    tiled = fits_tiles(devices, width) and slab_rows % 8 == 0 and track % lanes == 0 and width % lanes == 0
    tiled = tiled and components * layers % max(per_tile, 1) == 0
    tiled = tiled and 2 * components * layers <= slab_rows * max(per_tile, 1)
    return (local_tiled if tiled else local)(magnet, window_shift, region, material, kernel)


def solution(mesh):
    in_specs = (
        P(None, None, ("run", "gx", "gy"), None),
        P("run"),
        P(("run", "gx", "gy"), None),
        P(),
        P(None, None, ("gx", "gy"), None),
    )
    out_specs = (P(None, None, ("run", "gx", "gy"), None), P(None, None, ("run", "gx", "gy"), None))
    return jax.shard_map(local_any, mesh=mesh, in_specs=in_specs, out_specs=out_specs, check_vma=False)
```
